32 devices in a mesh: expert: 8 (over z, x), mp: 4 (over y, core).
Axes of the slice: x: 2, y: 2, z: 4, core: 2. Of those that a mesh axis runs over, the one named last changes fastest.
Arguments:
- tokens: bfloat16 [192, 6144], P('expert', 'mp'), may hold values from -6 to 6
- mix_weights: float32 [192, 2], P('expert'), may hold values from 0.2 to 1
- routes: int32 [192, 2], P('expert'), may hold values from 0 to 7, as said below
- w_gate: bfloat16 [8, 6144, 8192], P('expert', None, 'mp'), may hold values from -0.078125 to 0.078125
- w_up: bfloat16 [8, 6144, 8192], P('expert', None, 'mp'), may hold values from -0.078125 to 0.078125
- w_down: bfloat16 [8, 8192, 6144], P('expert', 'mp'), may hold values from -0.0625 to 0.0625
Outputs:
- mixed_out: bfloat16 [192, 6144], P('expert', 'mp')
The draws below stay inside these ranges and needn't reach their ends.
Inputs may be any that keep to these rules, and one draw needn't show every extreme that they name: `routes`: each row names 2 different experts, and every expert is named by some row. Among the 24 rows of one index of the expert axis no expert is named more than 12 times, and on some indices one is named exactly 12 times.
All inputs are finite; a program needn't handle non-finite values.
Results may differ from the reference program's by a relative error of at most 0.011.
Values may be sent and summed in bfloat16 or wider, within the bound.
A program may use at most 128 MiB of HBM per device.

```python
import jax
import jax.numpy as jnp

D = 6144
FF = 8192
EXPERTS = 8
TOP = 2
TOK_DEV = 24
MOST = 12
GROUP = 1
FF_SLICE = 8192
TOKENS = 192
CAP = 60


def block_routes(block_key, busiest):
    order_key, rows_key, shift_key = jax.random.split(block_key, 3)
    others_order = jax.random.permutation(order_key, EXPERTS - 1).astype(jnp.int32)
    others = ((busiest + 1 + others_order) % EXPERTS).astype(jnp.int32)
    row_order = jax.random.permutation(rows_key, TOK_DEV).astype(jnp.int32)
    shift = jax.random.randint(shift_key, (), 0, EXPERTS - 2).astype(jnp.int32)
    first = jnp.where(row_order < MOST, busiest, others[0]).astype(jnp.int32)
    second_idx = (1 + (row_order + shift) % (EXPERTS - 2)).astype(jnp.int32)
    second = jnp.take(others, second_idx).astype(jnp.int32)
    return jnp.stack([first, second], axis=1).astype(jnp.int32)


def draw_routes(key, part):
    base = jax.random.fold_in(key, 4711)
    busiest = jax.random.randint(jax.random.fold_in(base, 99), (), 0, EXPERTS).astype(jnp.int32)
    block_count = TOKENS // TOK_DEV
    keys = jax.random.split(base, block_count)
    grids = jax.vmap(block_routes, in_axes=(0, None))(keys, busiest)
    return grids.reshape(TOKENS, TOP).astype(jnp.int32)


def level_of(stream_key, dims, cuts, least, largest):
    factor_of = 1.0
    for axis_at, shards_of in cuts:
        heights = jax.random.uniform(jax.random.fold_in(jax.random.fold_in(stream_key, 6), axis_at), (shards_of,), jnp.float32, least / len(cuts), largest / len(cuts))
        factor_of = factor_of * jnp.repeat(jnp.exp(heights), dims[axis_at] // shards_of).reshape((-1,) + (1,) * (len(dims) - 1 - axis_at))
    return factor_of


def bell_draw(stream_key, extent, deviation, bound, shards=(), kind=jnp.bfloat16):
    result = deviation * jax.random.normal(stream_key, extent, jnp.float32)
    if shards:
        result = result * level_of(stream_key, extent, shards, -0.22, 0.18)
    return jnp.clip(result, -bound, bound).astype(kind)


def setup_inputs(seed: int = 0) -> dict:
    streams_of = jax.random.split(jax.random.key(seed), 7)
    return {
        "tokens": bell_draw(streams_of[0], (TOKENS, D), 1.0, 6.0, ((0, 8), (1, 4))),
        "mix_weights": jnp.clip(0.2 + 0.8 * jax.random.uniform(streams_of[1], (TOKENS, TOP), jnp.float32) ** level_of(streams_of[1], (TOKENS, TOP), ((0, 8),), -0.2, 0.2), 0.2, 1.0),
        "routes": draw_routes(jax.random.fold_in(streams_of[6], 71), 0),
        "w_gate": bell_draw(streams_of[3], (EXPERTS * GROUP, D, FF_SLICE), D ** -0.5, 0.078125, ((0, 8), (2, 4))),
        "w_up": bell_draw(streams_of[4], (EXPERTS * GROUP, D, FF_SLICE), D ** -0.5, 0.078125, ((0, 8), (2, 4))),
        "w_down": bell_draw(streams_of[5], (EXPERTS * GROUP, FF_SLICE, D), FF ** -0.5, 0.0625, ((0, 8), (1, 4))),
    }


def assignment_slots(routes):
    flat_ids = routes.reshape(-1)
    labels = jnp.arange(EXPERTS, dtype=jnp.int32)
    marked = (flat_ids[:, None] == labels[None, :]).astype(jnp.int32)
    earlier = jnp.cumsum(marked, axis=0) - marked
    return flat_ids, jnp.sum(earlier * marked, axis=1).astype(jnp.int32)


def reference(tokens, mix_weights, routes, w_gate, w_up, w_down):
    flat_ids, slot_ids = assignment_slots(routes)
    token_ids = (jnp.arange(TOKENS * TOP, dtype=jnp.int32) // TOP).astype(jnp.int32)
    slot_grid = slot_ids.reshape(TOKENS, TOP)
    mixed_out = jnp.zeros((TOKENS, D), jnp.float32)
    for expert in range(EXPERTS):
        chosen = (flat_ids == expert) & (slot_ids < CAP)
        target = jnp.where(chosen, slot_ids, CAP).astype(jnp.int32)
        holder = jnp.zeros((CAP + 1,), jnp.int32).at[target].set(token_ids)[:CAP]
        filled = jnp.zeros((CAP + 1,), jnp.int32).at[target].set(1)[:CAP]
        slot_rows = jnp.where(filled[:, None] > 0, tokens[holder], jnp.zeros((), tokens.dtype))
        expert_out = jnp.zeros((CAP, D), jnp.float32)
        for member in range(GROUP):
            weight_row = expert * GROUP + member
            gate_act = jnp.dot(slot_rows, w_gate[weight_row], preferred_element_type=jnp.float32)
            up_act = jnp.dot(slot_rows, w_up[weight_row], preferred_element_type=jnp.float32)
            hidden = (jax.nn.silu(gate_act) * up_act).astype(jnp.bfloat16)
            part_sum = jnp.dot(hidden, w_down[weight_row], preferred_element_type=jnp.float32).astype(jnp.bfloat16)
            expert_out = expert_out + part_sum.astype(jnp.float32)
        for column in range(TOP):
            is_taken = (routes[:, column] == expert) & (slot_grid[:, column] < CAP)
            weight = jnp.where(is_taken, mix_weights[:, column], jnp.zeros((), jnp.float32))
            picked = jnp.take(expert_out, jnp.minimum(slot_grid[:, column], CAP - 1).astype(jnp.int32), axis=0)
            mixed_out = mixed_out + weight[:, None] * picked
    return mixed_out.astype(jnp.bfloat16)
```

```python
import functools

import jax
import jax.numpy as jnp
from jax import lax
from jax.experimental import pallas as pl
from jax.experimental.pallas import tpu as pltpu
from jax.sharding import PartitionSpec as P

EXPERTS = 8
TOP = 2
STACK = 4
LANES = 128
SEG = STACK * LANES
TOKEN_PAD = 32
EXTRA = 4
ROUND_TO = 16
FAR_FIRST = (4, 3, 5, 2, 6, 1, 7)
MESH = pl.DeviceIdType.MESH
BF16, F32 = jnp.bfloat16, jnp.float32


def pass_order(chunks):
    arrival = (0, 12, 34, 45)
    pairs = [(which, c) for c in range(chunks) for which in range(4)]
    return sorted(pairs, key=lambda p: 21 * p[1] + arrival[p[0]])


def dot(a, b):
    return jnp.dot(a, b, preferred_element_type=F32)


def dot_nt(a, b):
    return lax.dot_general(a, b, (((1,), (1,)), ((), ())), preferred_element_type=F32)


def iota_f(shape, dim):
    return lax.broadcasted_iota(jnp.int32, shape, dim).astype(F32)


def split(index, size):
    high = jnp.floor((index + 0.5) * (1.0 / size))
    return high, index - high * size


def flag(cond):
    return jnp.where(cond, 1.0, 0.0)


def exchange(
    senders, capacity,
    tokens, mix, routes, w_gate, w_up, w_down, out,
    slots, tok, ids, mixw, packed, arrived, xbuf, acc, hidden, cnt_send, cnt_all,
    weighted, earlier_at, comp, spreader, weigh, own, pair_send, pair_recv,
    cross_send, cross_recv, ret_send, ret_recv,
):
    tok_rows, width = tokens.shape
    ff = w_gate.shape[2]
    chunks, cols_of = width // SEG, ff // SEG
    most = tok_rows // 2
    block = STACK * most
    stacked = senders * block
    n_slots = xbuf.shape[2]
    passes = pass_order(chunks)

    def body(
        w_sem, in_sem, cs_sem, cr_sem, as_sem, ar_sem, ss_sem, sr_sem, ys_sem, yr_sem,
        ps_sem, pr_sem, xs_sem, xr_sem, ts_sem, tr_sem,
    ):
        me = lax.axis_index("expert")
        m = lax.axis_index("mp")
        sibling = m + 1 - 2 * lax.rem(m, 2)
        across = lax.rem(m + 2, 4)
        across_sibling = lax.rem(sibling + 2, 4)
        order = (m, sibling, across, across_sibling)
        owners = (across_sibling, sibling, across, m)

        def peer(d):
            return lax.rem(me + d, senders)

        def remote(src, dst, send, recv, to_expert, to_mp):
            return pltpu.make_async_remote_copy(
                src_ref=src, dst_ref=dst, send_sem=send, recv_sem=recv,
                device_id=(to_expert, to_mp), device_id_type=MESH,
            )

        def weight_copy(i, up, b):
            which, c = passes[i]
            src = w_up if up else w_gate
            start = pl.multiple_of(order[which] * width + c * SEG, SEG)
            return pltpu.make_async_copy(
                src.at[0, pl.ds(start, SEG), pl.ds(b * SEG, SEG)],
                slots.at[2 * i + up, pl.ds(b * SEG, SEG), :],
                w_sem.at[2 * i + up, b],
            )

        def piece_slot(p):
            return 2 * len(passes) + p if p < EXTRA else p - EXTRA

        def piece_copy(p):
            start = pl.multiple_of(owners[p % 4] * width + (p // 4) * SEG, SEG)
            return pltpu.make_async_copy(
                w_down.at[0, :, pl.ds(start, SEG)], slots.at[piece_slot(p)], w_sem.at[piece_slot(p), 0]
            )

        barrier = pltpu.get_barrier_semaphore()
        for d in FAR_FIRST:
            pl.semaphore_signal(barrier, inc=1, device_id=(peer(d), m), device_id_type=MESH)
        for to in (across, across_sibling, sibling):
            pl.semaphore_signal(barrier, inc=1, device_id=(me, to), device_id_type=MESH)
        loads = (
            pltpu.make_async_copy(routes, ids, in_sem.at[0]),
            pltpu.make_async_copy(tokens, tok, in_sem.at[1]),
            pltpu.make_async_copy(mix, mixw, in_sem.at[2]),
        )
        for copy in loads:
            copy.start()
        for i in range(len(passes)):
            for up in range(2):
                for b in range(cols_of):
                    weight_copy(i, up, b).start(priority=1)
        for p in range(EXTRA):
            piece_copy(p).start(priority=1)

        row_e, row_rest = split(iota_f((stacked, tok_rows), 0), block)
        row_g, row_r = split(row_rest, most)
        upper = flag(iota_f((tok_rows, tok_rows), 0) < iota_f((tok_rows, tok_rows), 1)).astype(BF16)
        loads[0].wait()
        id_f = ids[...].astype(F32)
        first, second = flag(id_f[0:1, :] == row_e), flag(id_f[1:2, :] == row_e)
        marked = first + second
        earlier = dot(marked.astype(BF16), upper)
        sel = marked * flag(earlier == row_r)
        named = iota_f((LANES, tok_rows), 0)
        named = (flag(id_f[0:1, :] == named) + flag(id_f[1:2, :] == named)).astype(BF16)
        cnt_send[...] = dot_nt(jnp.ones((8, tok_rows), BF16), named)
        cnt_all[me] = cnt_send[...]
        loads[1].wait()
        loads[2].wait()
        total = None
        for j in range(STACK):
            segs = [tok[:, c * SEG + j * LANES : c * SEG + (j + 1) * LANES] for c in range(chunks)]
            part = dot((sel * flag(row_g == j)).astype(BF16), jnp.concatenate(segs, axis=1))
            total = part if total is None else total + part
        total = total.astype(BF16)
        for c in range(chunks):
            packed[c] = total[:, c * LANES : (c + 1) * LANES].reshape(senders, block, LANES)
            arrived[c, me] = packed[c, me]
        weights = mixw[...]
        weighted[...] = sel * (first * weights[0:1, :] + second * weights[1:2, :])
        earlier_at[...] = earlier

        def count_copy(d):
            return remote(cnt_send, cnt_all.at[me], cs_sem.at[d - 1], cr_sem.at[d - 1], peer(d), m)

        def block_copy(c, d):
            return remote(
                packed.at[c, peer(d)], arrived.at[c, me], as_sem.at[c, d - 1], ar_sem.at[c, d - 1], peer(d), m
            )

        def sibling_copy(c):
            return remote(xbuf.at[0, c], xbuf.at[1, c], ss_sem.at[0, c], sr_sem.at[0, c], me, sibling)

        def across_copy(c):
            return remote(xbuf.at[0, c], xbuf.at[2, c], ys_sem.at[c], yr_sem.at[c], me, across)

        def forward_copy(c):
            return remote(xbuf.at[2, c], xbuf.at[3, c], ss_sem.at[1, c], sr_sem.at[1, c], me, sibling)

        pl.semaphore_wait(barrier, senders - 1 + 3)
        for d in FAR_FIRST:
            count_copy(d).start()
        for c in range(chunks):
            for d in FAR_FIRST:
                block_copy(c, d).start()

        lane_e, lane_rest = split(iota_f((senders, stacked), 1), block)
        lane_g, lane_r = split(lane_rest[0:1, :], most)
        sender_at = iota_f((senders, stacked), 0)
        slot_j, slot_at = split(iota_f((STACK * n_slots, stacked), 0), n_slots)
        for d in range(1, senders):
            count_copy(d).wait_recv()
        counts = cnt_all[:, 0, :]
        lane_of = lax.broadcasted_iota(jnp.int32, (senders, LANES), 1)
        sender_of = lax.broadcasted_iota(jnp.int32, (senders, LANES), 0)
        mine = jnp.sum(jnp.where(lane_of == me, counts, 0.0), axis=1, keepdims=True)
        lane_cnt = jnp.sum(jnp.where(lane_e == sender_at, mine, 0.0), axis=0, keepdims=True)
        lane_off = jnp.sum(jnp.where(sender_at < lane_e, mine, 0.0), axis=0, keepdims=True)
        lane_slot = jnp.where(lane_r < lane_cnt, lane_off + lane_r, float(capacity))
        hit = flag(lane_slot == slot_at) * flag(lane_g == slot_j) * flag(slot_at < capacity)
        comp[...] = hit.astype(BF16)

        def prepare_return():
            spreader[...] = jnp.transpose(hit).astype(BF16)
            offset = jnp.sum(jnp.where(sender_of < me, counts, 0.0), axis=0, keepdims=True)
            of_row, _ = split(iota_f((stacked, LANES), 0), block)
            offset = jnp.sum(
                jnp.where(of_row == iota_f((stacked, LANES), 1), offset, 0.0), axis=1, keepdims=True
            )
            kept = weighted[...] * flag(offset + earlier_at[...] < capacity)
            high = kept.astype(BF16)
            low = (kept - high.astype(F32)).astype(BF16)
            _, token = split(iota_f((STACK * TOKEN_PAD, tok_rows), 0), TOKEN_PAD)
            spot = flag(token == iota_f((STACK * TOKEN_PAD, tok_rows), 1)).astype(BF16)
            seg, _ = split(iota_f((STACK * TOKEN_PAD, stacked), 0), TOKEN_PAD)
            there = flag(seg == lane_g)
            weigh[0] = (dot_nt(spot, high) * there).astype(BF16)
            weigh[1] = (dot_nt(spot, low) * there).astype(BF16)

        def take_chunk(c):
            for d in range(1, senders):
                block_copy(c, d).wait_recv()
            got = dot(comp[...], arrived[c].reshape(stacked, LANES)).astype(BF16)
            for j in range(STACK):
                xbuf[0, c, :, j * LANES : (j + 1) * LANES] = got[j * n_slots : (j + 1) * n_slots]
            across_copy(c).start()
            sibling_copy(c).start()

        prepare_return()
        for i, (which, c) in enumerate(passes):
            if which == 0:
                take_chunk(c)
            elif which == 1:
                sibling_copy(c).wait_recv()
            elif which == 2:
                across_copy(c).wait_recv()
                forward_copy(c).start()
            else:
                forward_copy(c).wait_recv()
            for up in range(2):
                for b in range(cols_of):
                    weight_copy(i, up, b).wait()
            x = xbuf[which, c]
            last = i == len(passes) - 1
            for b in range(cols_of):
                at = slice(b * SEG, (b + 1) * SEG)
                both = [dot(x, slots[2 * i + up, at, :]) for up in range(2)]
                if i:
                    both = [acc[up, :, at] + both[up] for up in range(2)]
                if last:
                    gate, up_act = both
                    hidden[:, at] = (gate / (1.0 + jnp.exp(-gate)) * up_act).astype(BF16)
                else:
                    acc[0, :, at], acc[1, :, at] = both
            for p in range(EXTRA + 2 * i, min(EXTRA + 2 * i + 2, 4 * chunks)):
                piece_copy(p).start(priority=1)

        def pair_copy(c):
            return remote(pair_send.at[c], pair_recv.at[c], ps_sem.at[c], pr_sem.at[c], me, sibling)

        def cross_copy(c):
            return remote(cross_send.at[c], cross_recv.at[c], xs_sem.at[c], xr_sem.at[c], me, across)

        def return_copy(c, d):
            return remote(
                ret_send.at[c, peer(d)], ret_recv.at[c, me], ts_sem.at[c, d - 1], tr_sem.at[c, d - 1], peer(d), m
            )

        def piece(c, o):
            piece_copy(4 * c + o).wait()
            return dot(hidden[...], slots[piece_slot(4 * c + o)])

        def send_back(c):
            cross_copy(c).wait_recv()
            total = (own[c] + cross_recv[c].astype(F32)).astype(BF16)
            total = jnp.concatenate([total[:, j * LANES : (j + 1) * LANES] for j in range(STACK)], axis=0)
            ret_send[c] = dot(spreader[...], total).astype(BF16).reshape(senders, block, LANES)
            ret_recv[c, me] = ret_send[c, me]
            for d in FAR_FIRST:
                return_copy(c, d).start()

        for c in range(chunks):
            pair_send[c, 0] = piece(c, 0).astype(BF16)
            pair_send[c, 1] = piece(c, 1).astype(BF16)
            pair_copy(c).start()
            if c:
                send_back(c - 1)
            cross = piece(c, 2)
            own[c] = piece(c, 3)
            pair_copy(c).wait_recv()
            cross_send[c] = (cross + pair_recv[c, 0].astype(F32)).astype(BF16)
            cross_copy(c).start()
            own[c] = own[c] + pair_recv[c, 1].astype(F32)
        send_back(chunks - 1)

        for c in range(chunks):
            for d in range(1, senders):
                return_copy(c, d).wait_recv()
            rows = ret_recv[c].reshape(stacked, LANES)
            mixed = (dot(weigh[0], rows) + dot(weigh[1], rows)).astype(BF16)
            for j in range(STACK):
                at = c * SEG + j * LANES
                out[:, at : at + LANES] = mixed[j * TOKEN_PAD : j * TOKEN_PAD + tok_rows]

        for d in range(1, senders):
            count_copy(d).wait_send()
        for c in range(chunks):
            for d in range(1, senders):
                block_copy(c, d).wait_send()
                return_copy(c, d).wait_send()
            across_copy(c).wait_send()
            sibling_copy(c).wait_send()
            forward_copy(c).wait_send()
            pair_copy(c).wait_send()
            cross_copy(c).wait_send()

    dma = pltpu.SemaphoreType.DMA
    others = senders - 1
    pl.run_scoped(
        body,
        dma((slots.shape[0], cols_of)), dma((3,)),
        dma((others,)), dma((others,)),
        dma((chunks, others)), dma((chunks, others)),
        dma((2, chunks)), dma((2, chunks)),
        dma((chunks,)), dma((chunks,)),
        dma((chunks,)), dma((chunks,)),
        dma((chunks,)), dma((chunks,)),
        dma((chunks, others)), dma((chunks, others)),
    )


def local_fused(tokens, mix_weights, routes, w_gate, w_up, w_down):
    tok_rows, width = tokens.shape
    senders = lax.axis_size("expert")
    capacity = 5 * tok_rows * senders * TOP // (4 * EXPERTS)
    n_slots = -(-capacity // ROUND_TO) * ROUND_TO
    ff = w_gate.shape[2]
    chunks = width // SEG
    block = STACK * (tok_rows // 2)
    stacked = senders * block
    vmem = pl.BlockSpec(memory_space=pltpu.VMEM)
    hbm = pl.BlockSpec(memory_space=pl.ANY)
    return pl.pallas_call(
        functools.partial(exchange, senders, capacity),
        out_shape=jax.ShapeDtypeStruct((tok_rows, width), BF16),
        in_specs=[hbm] * 6,
        out_specs=vmem,
        scratch_shapes=[
            pltpu.VMEM((8 * chunks + EXTRA, ff, SEG), BF16),
            pltpu.VMEM((tok_rows, width), BF16),
            pltpu.VMEM((TOP, tok_rows), jnp.int32),
            pltpu.VMEM((TOP, tok_rows), F32),
            pltpu.VMEM((chunks, senders, block, LANES), BF16),
            pltpu.VMEM((chunks, senders, block, LANES), BF16),
            pltpu.VMEM((4, chunks, n_slots, SEG), BF16),
            pltpu.VMEM((2, n_slots, ff), F32),
            pltpu.VMEM((n_slots, ff), BF16),
            pltpu.VMEM((8, LANES), F32),
            pltpu.VMEM((senders, 8, LANES), F32),
            pltpu.VMEM((stacked, tok_rows), F32),
            pltpu.VMEM((stacked, tok_rows), F32),
            pltpu.VMEM((STACK * n_slots, stacked), BF16),
            pltpu.VMEM((stacked, STACK * n_slots), BF16),
            pltpu.VMEM((2, STACK * TOKEN_PAD, stacked), BF16),
            pltpu.VMEM((chunks, n_slots, SEG), F32),
            pltpu.VMEM((chunks, 2, n_slots, SEG), BF16),
            pltpu.VMEM((chunks, 2, n_slots, SEG), BF16),
            pltpu.VMEM((chunks, n_slots, SEG), BF16),
            pltpu.VMEM((chunks, n_slots, SEG), BF16),
            pltpu.VMEM((chunks, senders, block, LANES), BF16),
            pltpu.VMEM((chunks, senders, block, LANES), BF16),
        ],
        compiler_params=pltpu.CompilerParams(
            collective_id=0, has_side_effects=True, vmem_limit_bytes=67_043_328
        ),
    )(tokens, mix_weights.T, routes.T, w_gate, w_up, w_down)


def fits(tokens, w_gate):
    senders, ways = lax.axis_size("expert"), lax.axis_size("mp")
    tok_rows, width = tokens.shape
    depth, ff = w_gate.shape[1], w_gate.shape[2]
    return (
        senders == EXPERTS
        and ways == 4
        and tok_rows % 8 == 0
        and (STACK * (tok_rows // 2)) % 16 == 0
        and tok_rows <= TOKEN_PAD
        and depth == 4 * width
        and width % SEG == 0
        and ff == STACK * SEG
        and (8 * (width // SEG) + EXTRA) * ff * SEG * 2 <= 58_800_000
    )


def local_any(tokens, mix_weights, routes, w_gate, w_up, w_down):
    form = local_fused if fits(tokens, w_gate) else local
    return form(tokens, mix_weights, routes, w_gate, w_up, w_down)


def pack_rows(pick_tokens, features, repeats):
    packed = jnp.einsum(
        "tem,tc->emc", pick_tokens, features, preferred_element_type=jnp.float32
    ).astype(jnp.bfloat16)
    spread = jnp.broadcast_to(packed[:, None], (packed.shape[0], repeats) + packed.shape[1:])
    return spread.reshape((packed.shape[0] * repeats,) + packed.shape[1:])


def activate(gate_act, up_act):
    return (jax.nn.silu(gate_act) * up_act).astype(jnp.bfloat16)


def local(tokens, mix_weights, routes, w_gate, w_up, w_down):
    tok_rows = tokens.shape[0]
    senders = lax.axis_size("expert")
    group_size = senders // EXPERTS
    capacity = 5 * tok_rows * senders * TOP // (4 * EXPERTS)
    most_rows = tok_rows // 2
    labels = jnp.arange(EXPERTS, dtype=jnp.int32)
    flat_ids = routes.reshape(-1)
    marked = (flat_ids[:, None] == labels[None, :]).astype(jnp.int32)
    earlier = jnp.cumsum(marked, axis=0) - marked
    local_rank = jnp.sum(earlier * marked, axis=1)
    counts = jnp.sum(marked, axis=0)
    count_grid = lax.all_gather(counts[None, :], "expert", axis=0, tiled=True)
    my_index = lax.axis_index("expert")
    sender_ids = jnp.arange(senders, dtype=jnp.int32)
    lower_mask = (sender_ids[:, None] < my_index).astype(jnp.int32)
    offsets = jnp.sum(count_grid * lower_mask, axis=0)
    slot_ids = jnp.sum(marked * offsets[None, :], axis=1) + local_rank
    keep_mask = (slot_ids < capacity).astype(jnp.int32)
    rank_hit = (local_rank[:, None] == jnp.arange(most_rows, dtype=jnp.int32)[None, :]).astype(
        jnp.int32
    ) * keep_mask[:, None]
    assign_pick = marked[:, :, None] * rank_hit[:, None, :]
    pick_tokens = jnp.sum(assign_pick.reshape(tok_rows, TOP, EXPERTS, most_rows), axis=1).astype(
        jnp.bfloat16
    )
    weighted = assign_pick.astype(jnp.float32) * mix_weights.reshape(-1)[:, None, None]
    combine_w = jnp.sum(weighted.reshape(tok_rows, TOP, EXPERTS * most_rows), axis=1)
    gate_rows = w_gate[0]
    up_rows = w_up[0]
    down_rows = w_down[0]
    arrived = lax.all_to_all(
        pack_rows(pick_tokens, tokens, group_size),
        "expert",
        split_axis=0,
        concat_axis=0,
        tiled=True,
    )
    arrived_rows = arrived.reshape(senders * most_rows, arrived.shape[2])
    shard_piece = lax.all_gather(arrived_rows, "mp", axis=1, tiled=True)
    gate_act = jnp.dot(shard_piece, gate_rows, preferred_element_type=jnp.float32)
    up_act = jnp.dot(shard_piece, up_rows, preferred_element_type=jnp.float32)
    hidden = activate(gate_act, up_act)
    part_sum = jnp.dot(hidden, down_rows, preferred_element_type=jnp.float32)
    reduced = lax.psum_scatter(part_sum, "mp", scatter_dimension=1, tiled=True).astype(jnp.bfloat16)
    out_width = reduced.shape[1]
    returned = lax.all_to_all(
        reduced.reshape(senders, most_rows, out_width),
        "expert",
        split_axis=0,
        concat_axis=0,
        tiled=True,
    )
    summed = jnp.sum(
        returned.reshape(EXPERTS, group_size, most_rows, out_width).astype(jnp.float32), axis=1
    )
    result = jnp.dot(
        combine_w, summed.reshape(EXPERTS * most_rows, out_width), precision=lax.Precision.HIGHEST
    )
    return result.astype(jnp.bfloat16)


def solution(mesh):
    placed = (
        P("expert", "mp"),
        P("expert", None),
        P("expert", None),
        P("expert", None, "mp"),
        P("expert", None, "mp"),
        P("expert", "mp", None),
    )
    return jax.shard_map(
        local_any, mesh=mesh, in_specs=placed, out_specs=P("expert", "mp"), check_vma=False
    )
```

```python
import functools

import jax
import jax.numpy as jnp
from jax import lax
from jax.experimental import pallas as pl
from jax.experimental.pallas import tpu as pltpu
from jax.sharding import PartitionSpec as P

EXPERTS = 8
TOP = 2
STACK = 4
LANES = 128
SEG = STACK * LANES
BACK = 2
UNIT = BACK * LANES
TOKEN_PAD = 32
RING = 22
ROUND_TO = 16
FAR_FIRST = (7, 6, 5, 4, 3, 2, 1)
MESH = pl.DeviceIdType.MESH
BF16, F32 = jnp.bfloat16, jnp.float32


def schedule(chunks):
    last = chunks - 1
    events = []
    for c in range(last):
        events += [("do", 0, c), ("wait", 0, c), ("group", (0, c))] + ([] if c else [("prepare",)])
    events += [("do", 1, 0), ("do", 2, 0), ("do", 0, last)]
    events += [("do", 1, c) for c in range(1, last)] + [("wait", 0, last), ("group", (0, last))]
    events += [("do", 1, last)]
    for c in range(chunks):
        events += [("wait", 1, c)] + ([("do", 2, c + 1)] if c < last else [])
        events += [("do", 3, c - 1)] if c else []
        events += [("wait", 2, c), ("group", (1, c), (2, c))]
    events += [("do", 3, last), *(("wait", 3, c) for c in range(last))]
    events += [("group", *((3, c) for c in range(last)))]
    events += [("wait", 3, last), ("group", (3, last))]
    return events


def down_order(units):
    ahead = min(3, units)
    order = [(0, u) for u in range(ahead)]
    for u in range(units):
        order += [(1, u)] + ([(0, u + ahead)] if u + ahead < units else [])
    return order


def piece_order(chunks):
    first_use = {}
    for half, unit in down_order(2 * chunks):
        for owner in (2 * half, 2 * half + 1):
            first_use.setdefault((owner, unit // 2), None)
    return list(first_use)


def dot(a, b):
    return jnp.dot(a, b, preferred_element_type=F32)


def dot_nt(a, b):
    return lax.dot_general(a, b, (((1,), (1,)), ((), ())), preferred_element_type=F32)


def iota_f(shape, dim):
    return lax.broadcasted_iota(jnp.int32, shape, dim).astype(F32)


def split(index, size):
    high = jnp.floor((index + 0.5) * (1.0 / size))
    return high, index - high * size


def flag(cond):
    return jnp.where(cond, 1.0, 0.0)


def exchange(
    senders, capacity,
    tokens, mix, routes, w_gate, w_up, w_down, out,
    slots, tok, ids, mixw, packed, arrived, xbuf, acc, hidden, cnt_send, cnt_all,
    weighted, earlier_at, comp, spreader, weigh, own, pair_send, pair_recv,
    cross_send, cross_recv, ret_send, ret_recv,
):
    tok_rows, width = tokens.shape
    ff = w_gate.shape[2]
    chunks, cols_of, units = width // SEG, ff // SEG, width // UNIT
    most = tok_rows // 2
    block = STACK * most
    stacked = senders * block
    back_block = BACK * most
    back_rows = senders * back_block
    n_slots = xbuf.shape[2]
    events = schedule(chunks)
    passes = [part for event in events if event[0] == "group" for part in event[1:]]
    pieces = piece_order(chunks)
    ring = slots.shape[0]
    loads = 2 * len(passes) + len(pieces)

    def body(
        w_sem, in_sem, cs_sem, cr_sem, as_sem, ar_sem, ss_sem, sr_sem, ys_sem, yr_sem,
        ps_sem, pr_sem, xs_sem, xr_sem, ts_sem, tr_sem,
    ):
        me = lax.axis_index("expert")
        m = lax.axis_index("mp")
        sibling = m + 1 - 2 * lax.rem(m, 2)
        across = lax.rem(m + 2, 4)
        across_sibling = lax.rem(sibling + 2, 4)
        odd = lax.rem(m, 2)
        base = m - odd
        sources = (base + 1, base, lax.rem(base + 3, 4), lax.rem(base + 2, 4))
        held_at = (1 - odd, odd, 3 - odd, 2 + odd)
        owners = (across_sibling, across, sibling, m)

        bits = (lax.rem(me, 2), lax.rem(me // 2, 2), me // 4)

        def peer(d):
            return sum((1 - bit if d >> i & 1 else bit) * (1 << i) for i, bit in enumerate(bits))

        def remote(src, dst, send, recv, to_expert, to_mp):
            return pltpu.make_async_remote_copy(
                src_ref=src, dst_ref=dst, send_sem=send, recv_sem=recv,
                device_id=(to_expert, to_mp), device_id_type=MESH,
            )

        def copies(k):
            if k >= 2 * len(passes):
                owner, c = pieces[k - 2 * len(passes)]
                start = pl.multiple_of(owners[owner] * width + c * SEG, SEG)
                return [pltpu.make_async_copy(w_down.at[0, :, pl.ds(start, SEG)], slots.at[k % ring], w_sem.at[k % ring, 0])]
            source, c = passes[k // 2]
            src = w_up if k % 2 else w_gate
            start = pl.multiple_of(sources[source] * width + c * SEG, SEG)
            return [
                pltpu.make_async_copy(
                    src.at[0, pl.ds(start, SEG), pl.ds(b * SEG, SEG)],
                    slots.at[k % ring, pl.ds(b * SEG, SEG), :],
                    w_sem.at[k % ring, b],
                )
                for b in range(cols_of)
            ]

        def fetch(k):
            if k < loads:
                for copy in copies(k):
                    copy.start(priority=1)

        def fetched(k):
            for copy in copies(k):
                copy.wait()

        small = (
            pltpu.make_async_copy(routes, ids, in_sem.at[0]),
            pltpu.make_async_copy(tokens, tok, in_sem.at[1]),
            pltpu.make_async_copy(mix, mixw, in_sem.at[2]),
        )
        for copy in small:
            copy.start()
        barrier = pltpu.get_barrier_semaphore()
        for d in FAR_FIRST:
            pl.semaphore_signal(barrier, inc=1, device_id=(peer(d), m), device_id_type=MESH)
        for to in (across, across_sibling, sibling):
            pl.semaphore_signal(barrier, inc=1, device_id=(me, to), device_id_type=MESH)
        for k in range(ring):
            fetch(k)

        row_e, row_rest = split(iota_f((stacked, tok_rows), 0), block)
        row_g, row_r = split(row_rest, most)
        upper = flag(iota_f((tok_rows, tok_rows), 0) < iota_f((tok_rows, tok_rows), 1)).astype(BF16)
        small[0].wait()
        id_f = ids[...].astype(F32)
        first, second = flag(id_f[0:1, :] == row_e), flag(id_f[1:2, :] == row_e)
        marked = first + second
        earlier = dot(marked.astype(BF16), upper)
        sel = marked * flag(earlier == row_r)
        named = iota_f((LANES, tok_rows), 0)
        named = (flag(id_f[0:1, :] == named) + flag(id_f[1:2, :] == named)).astype(BF16)
        cnt_send[...] = dot_nt(jnp.ones((8, tok_rows), BF16), named)
        cnt_all[me] = cnt_send[...]
        small[1].wait()
        small[2].wait()
        total = None
        for j in range(STACK):
            segs = [tok[:, c * SEG + j * LANES : c * SEG + (j + 1) * LANES] for c in range(chunks)]
            part = dot((sel * flag(row_g == j)).astype(BF16), jnp.concatenate(segs, axis=1))
            total = part if total is None else total + part
        total = total.astype(BF16)
        for c in range(chunks):
            packed[c] = total[:, c * LANES : (c + 1) * LANES].reshape(senders, block, LANES)
            arrived[c, me] = packed[c, me]
        weights = mixw[...]
        weighted[...] = sel * (first * weights[0:1, :] + second * weights[1:2, :])
        earlier_at[...] = earlier

        def count_copy(d):
            return remote(cnt_send, cnt_all.at[me], cs_sem.at[d - 1], cr_sem.at[d - 1], peer(d), m)

        def block_copy(c, d):
            return remote(
                packed.at[c, peer(d)], arrived.at[c, me], as_sem.at[c, d - 1], ar_sem.at[c, d - 1], peer(d), m
            )

        def sibling_copy(c):
            return remote(xbuf.at[0, c], xbuf.at[1, c], ss_sem.at[0, c], sr_sem.at[0, c], me, sibling)

        def across_copy(c):
            return remote(xbuf.at[0, c], xbuf.at[2, c], ys_sem.at[c], yr_sem.at[c], me, across)

        def forward_copy(c):
            return remote(xbuf.at[2, c], xbuf.at[3, c], ss_sem.at[1, c], sr_sem.at[1, c], me, sibling)

        pl.semaphore_wait(barrier, senders - 1 + 3)
        for d in FAR_FIRST:
            count_copy(d).start()
        for c in range(chunks):
            for d in FAR_FIRST:
                block_copy(c, d).start()

        for d in range(1, senders):
            count_copy(d).wait_recv()
        counts = cnt_all[:, 0, :]
        lane_of = lax.broadcasted_iota(jnp.int32, (senders, LANES), 1)
        sender_of = lax.broadcasted_iota(jnp.int32, (senders, LANES), 0)
        mine = jnp.sum(jnp.where(lane_of == me, counts, 0.0), axis=1, keepdims=True)

        def placed(stack):
            count = senders * stack * most
            lane_e, lane_rest = split(iota_f((senders, count), 1), stack * most)
            lane_g, lane_r = split(lane_rest[0:1, :], most)
            sender_at = iota_f((senders, count), 0)
            lane_cnt = jnp.sum(jnp.where(lane_e == sender_at, mine, 0.0), axis=0, keepdims=True)
            lane_off = jnp.sum(jnp.where(sender_at < lane_e, mine, 0.0), axis=0, keepdims=True)
            lane_slot = jnp.where(lane_r < lane_cnt, lane_off + lane_r, float(capacity))
            slot_j, slot_at = split(iota_f((stack * n_slots, count), 0), n_slots)
            hit = flag(lane_slot == slot_at) * flag(lane_g == slot_j) * flag(slot_at < capacity)
            return hit.astype(BF16), lane_g

        comp[...] = placed(STACK)[0]

        def prepare_return():
            hit, lane_g = placed(BACK)
            eye = flag(iota_f((back_rows, back_rows), 0) == iota_f((back_rows, back_rows), 1))
            spreader[...] = dot_nt(eye.astype(BF16), hit).astype(BF16)
            offset = jnp.sum(jnp.where(sender_of < me, counts, 0.0), axis=0, keepdims=True)
            of_row, _ = split(iota_f((back_rows, LANES), 0), back_block)
            offset = jnp.sum(
                jnp.where(of_row == iota_f((back_rows, LANES), 1), offset, 0.0), axis=1, keepdims=True
            )
            whole, ahead = (
                at[...].reshape(senders, block, tok_rows)[:, :back_block].reshape(back_rows, tok_rows)
                for at in (weighted, earlier_at)
            )
            kept = whole * flag(offset + ahead < capacity)
            high = kept.astype(BF16)
            low = (kept - high.astype(F32)).astype(BF16)
            _, token = split(iota_f((BACK * TOKEN_PAD, tok_rows), 0), TOKEN_PAD)
            spot = flag(token == iota_f((BACK * TOKEN_PAD, tok_rows), 1)).astype(BF16)
            seg, _ = split(iota_f((BACK * TOKEN_PAD, back_rows), 0), TOKEN_PAD)
            there = flag(seg == lane_g)
            weigh[0] = (dot_nt(spot, high) * there).astype(BF16)
            weigh[1] = (dot_nt(spot, low) * there).astype(BF16)

        def take_chunk(c):
            for d in range(1, senders):
                block_copy(c, d).wait_recv()
            got = dot(comp[...], arrived[c].reshape(stacked, LANES)).astype(BF16)
            for j in range(STACK):
                xbuf[0, c, :, j * LANES : (j + 1) * LANES] = got[j * n_slots : (j + 1) * n_slots]
            across_copy(c).start()
            sibling_copy(c).start()

        def do(source, c):
            if source < 2:
                take_chunk(c)
            else:
                across_copy(c).wait_recv()
                forward_copy(c).start()

        def wait(source, c):
            (sibling_copy if source < 2 else forward_copy)(c).wait_recv()

        def group(parts, start, first, last):
            for k in range(2 * start, 2 * (start + len(parts))):
                fetched(k)
            xs = [xbuf[held_at[source], c] for source, c in parts]
            for b in range(cols_of):
                at = slice(b * SEG, (b + 1) * SEG)
                both = [
                    sum(dot(x, slots[(2 * (start + i) + up) % ring, at, :]) for i, x in enumerate(xs)) for up in range(2)
                ]
                if not first:
                    both = [acc[up, :, at] + both[up] for up in range(2)]
                if last:
                    gate, up_act = both
                    hidden[:, at] = (gate / (1.0 + jnp.exp(-gate)) * up_act).astype(BF16)
                else:
                    acc[0, :, at], acc[1, :, at] = both
            for k in range(2 * start, 2 * (start + len(parts))):
                fetch(k + ring)

        done = 0
        for event in events:
            if event[0] == "prepare":
                prepare_return()
            elif event[0] == "group":
                parts = event[1:]
                group(parts, done, done == 0, done + len(parts) == len(passes))
                done += len(parts)
            else:
                kind, source, c = event
                acts = odd == (1 - source % 2 if kind == "do" else source % 2)
                pl.when(acts)(functools.partial(do if kind == "do" else wait, source, c))

        def pair_copy(o, c):
            return remote(
                pair_send.at[o, c], pair_recv.at[o, c], ps_sem.at[o, c], pr_sem.at[o, c], me, sibling
            )

        def cross_copy(c):
            return remote(cross_send.at[c], cross_recv.at[c], xs_sem.at[c], xr_sem.at[c], me, across)

        def return_copy(c, d):
            return remote(
                ret_send.at[c, peer(d)], ret_recv.at[c, me], ts_sem.at[c, d - 1], tr_sem.at[c, d - 1], peer(d), m
            )

        def down_block(half, u):
            at = [2 * len(passes) + pieces.index((2 * half + i, u // 2)) for i in range(2)]
            if u % 2 == 0:
                for k in at:
                    fetched(k)
            cols = slice(u % 2 * UNIT, (u % 2 + 1) * UNIT)
            return [dot(hidden[...], slots[k % ring, :, cols]) for k in at]

        def cross_step(c):
            pair_copy(0, c).wait_recv()
            cross_send[c] = (own[0, c] + pair_recv[0, c].astype(F32)).astype(BF16)
            cross_copy(c).start()

        def send_back(c):
            pair_copy(1, c).wait_recv()
            cross_copy(c).wait_recv()
            total = own[1, c] + pair_recv[1, c].astype(F32) + cross_recv[c].astype(F32)
            total = total.astype(BF16)
            total = jnp.concatenate([total[:, j * LANES : (j + 1) * LANES] for j in range(BACK)], axis=0)
            ret_send[c] = dot(spreader[...], total).reshape(senders, back_block, LANES).astype(BF16)
            ret_recv[c, me] = ret_send[c, me]
            for d in FAR_FIRST:
                return_copy(c, d).start()

        order = down_order(units)
        crossing = {order.index((0, u)) + 2: u for u in range(units)}
        returning = {}
        for u in range(units):
            returning.setdefault(min(max(order.index((0, u)) + 7, order.index((1, u)) + 2), len(order)), []).append(u)
        for i, (half, u) in enumerate(order):
            there, own[half, u] = down_block(half, u)
            pair_send[half, u] = there.astype(BF16)
            pair_copy(half, u).start()
            if i in crossing:
                cross_step(crossing[i])
            for back in returning.get(i, ()):
                send_back(back)
        for back in returning.get(len(order), ()):
            send_back(back)

        for u in range(units):
            for d in range(1, senders):
                return_copy(u, d).wait_recv()
            rows = ret_recv[u].astype(F32).reshape(back_rows, LANES).astype(BF16)
            mixed = (dot(weigh[0], rows) + dot(weigh[1], rows)).astype(BF16)
            for j in range(BACK):
                at = u * UNIT + j * LANES
                out[:, at : at + LANES] = mixed[j * TOKEN_PAD : j * TOKEN_PAD + tok_rows]

        for d in range(1, senders):
            count_copy(d).wait_send()
        for c in range(chunks):
            for d in range(1, senders):
                block_copy(c, d).wait_send()
            across_copy(c).wait_send()
            sibling_copy(c).wait_send()
            forward_copy(c).wait_send()
        for u in range(units):
            for d in range(1, senders):
                return_copy(u, d).wait_send()
            pair_copy(0, u).wait_send()
            pair_copy(1, u).wait_send()
            cross_copy(u).wait_send()

    dma = pltpu.SemaphoreType.DMA
    others = senders - 1
    pl.run_scoped(
        body,
        dma((slots.shape[0], cols_of)), dma((3,)),
        dma((others,)), dma((others,)),
        dma((chunks, others)), dma((chunks, others)),
        dma((2, chunks)), dma((2, chunks)),
        dma((chunks,)), dma((chunks,)),
        dma((2, units)), dma((2, units)),
        dma((units,)), dma((units,)),
        dma((units, others)), dma((units, others)),
    )


def local_fused(tokens, mix_weights, routes, w_gate, w_up, w_down):
    tok_rows, width = tokens.shape
    senders = lax.axis_size("expert")
    capacity = 5 * tok_rows * senders * TOP // (4 * EXPERTS)
    n_slots = -(-capacity // ROUND_TO) * ROUND_TO
    ff = w_gate.shape[2]
    chunks = width // SEG
    block = STACK * (tok_rows // 2)
    stacked = senders * block
    units, back_rows = width // UNIT, senders * BACK * (tok_rows // 2)
    vmem = pl.BlockSpec(memory_space=pltpu.VMEM)
    hbm = pl.BlockSpec(memory_space=pltpu.HBM)
    return pl.pallas_call(
        functools.partial(exchange, senders, capacity),
        out_shape=jax.ShapeDtypeStruct((tok_rows, width), BF16),
        in_specs=[hbm] * 6,
        out_specs=vmem,
        scratch_shapes=[
            pltpu.VMEM((RING, ff, SEG), BF16),
            pltpu.VMEM((tok_rows, width), BF16),
            pltpu.VMEM((TOP, tok_rows), jnp.int32),
            pltpu.VMEM((TOP, tok_rows), F32),
            pltpu.VMEM((chunks, senders, block, LANES), BF16),
            pltpu.VMEM((chunks, senders, block, LANES), BF16),
            pltpu.VMEM((4, chunks, n_slots, SEG), BF16),
            pltpu.VMEM((2, n_slots, ff), F32),
            pltpu.VMEM((n_slots, ff), BF16),
            pltpu.VMEM((8, LANES), F32),
            pltpu.VMEM((senders, 8, LANES), F32),
            pltpu.VMEM((stacked, tok_rows), F32),
            pltpu.VMEM((stacked, tok_rows), F32),
            pltpu.VMEM((STACK * n_slots, stacked), BF16),
            pltpu.VMEM((back_rows, BACK * n_slots), BF16),
            pltpu.VMEM((2, BACK * TOKEN_PAD, back_rows), BF16),
            pltpu.VMEM((2, units, n_slots, UNIT), F32),
            pltpu.VMEM((2, units, n_slots, UNIT), BF16),
            pltpu.VMEM((2, units, n_slots, UNIT), BF16),
            pltpu.VMEM((units, n_slots, UNIT), BF16),
            pltpu.VMEM((units, n_slots, UNIT), BF16),
            pltpu.VMEM((units, senders, back_rows // senders, LANES), BF16),
            pltpu.VMEM((units, senders, back_rows // senders, LANES), BF16),
        ],
        compiler_params=pltpu.CompilerParams(
            collective_id=0, has_side_effects=True, vmem_limit_bytes=54_000_000
        ),
    )(*(pltpu.with_memory_space_constraint(a, pltpu.HBM) for a in (tokens, mix_weights.T, routes.T, w_gate, w_up, w_down)))


def fits(tokens, w_gate):
    senders, ways = lax.axis_size("expert"), lax.axis_size("mp")
    tok_rows, width = tokens.shape
    depth, ff = w_gate.shape[1], w_gate.shape[2]
    return (
        senders == EXPERTS
        and ways == 4
        and tok_rows % 8 == 0
        and (STACK * (tok_rows // 2)) % 16 == 0
        and (BACK * (tok_rows // 2)) % 8 == 0
        and tok_rows <= TOKEN_PAD
        and depth == 4 * width
        and width % SEG == 0
        and ff == STACK * SEG
        and width // SEG > 1
        and RING * ff * SEG * 2 <= 47_000_000
    )


def local_any(tokens, mix_weights, routes, w_gate, w_up, w_down):
    form = local_fused if fits(tokens, w_gate) else local
    return form(tokens, mix_weights, routes, w_gate, w_up, w_down)


def pack_rows(pick_tokens, features, repeats):
    packed = jnp.einsum(
        "tem,tc->emc", pick_tokens, features, preferred_element_type=jnp.float32
    ).astype(jnp.bfloat16)
    spread = jnp.broadcast_to(packed[:, None], (packed.shape[0], repeats) + packed.shape[1:])
    return spread.reshape((packed.shape[0] * repeats,) + packed.shape[1:])


def activate(gate_act, up_act):
    return (jax.nn.silu(gate_act) * up_act).astype(jnp.bfloat16)


def local(tokens, mix_weights, routes, w_gate, w_up, w_down):
    tok_rows = tokens.shape[0]
    senders = lax.axis_size("expert")
    group_size = senders // EXPERTS
    capacity = 5 * tok_rows * senders * TOP // (4 * EXPERTS)
    most_rows = tok_rows // 2
    labels = jnp.arange(EXPERTS, dtype=jnp.int32)
    flat_ids = routes.reshape(-1)
    marked = (flat_ids[:, None] == labels[None, :]).astype(jnp.int32)
    earlier = jnp.cumsum(marked, axis=0) - marked
    local_rank = jnp.sum(earlier * marked, axis=1)
    counts = jnp.sum(marked, axis=0)
    count_grid = lax.all_gather(counts[None, :], "expert", axis=0, tiled=True)
    my_index = lax.axis_index("expert")
    sender_ids = jnp.arange(senders, dtype=jnp.int32)
    lower_mask = (sender_ids[:, None] < my_index).astype(jnp.int32)
    offsets = jnp.sum(count_grid * lower_mask, axis=0)
    slot_ids = jnp.sum(marked * offsets[None, :], axis=1) + local_rank
    keep_mask = (slot_ids < capacity).astype(jnp.int32)
    rank_hit = (local_rank[:, None] == jnp.arange(most_rows, dtype=jnp.int32)[None, :]).astype(
        jnp.int32
    ) * keep_mask[:, None]
    assign_pick = marked[:, :, None] * rank_hit[:, None, :]
    pick_tokens = jnp.sum(assign_pick.reshape(tok_rows, TOP, EXPERTS, most_rows), axis=1).astype(
        jnp.bfloat16
    )
    weighted = assign_pick.astype(jnp.float32) * mix_weights.reshape(-1)[:, None, None]
    combine_w = jnp.sum(weighted.reshape(tok_rows, TOP, EXPERTS * most_rows), axis=1)
    gate_rows = w_gate[0]
    up_rows = w_up[0]
    down_rows = w_down[0]
    arrived = lax.all_to_all(
        pack_rows(pick_tokens, tokens, group_size),
        "expert",
        split_axis=0,
        concat_axis=0,
        tiled=True,
    )
    arrived_rows = arrived.reshape(senders * most_rows, arrived.shape[2])
    shard_piece = lax.all_gather(arrived_rows, "mp", axis=1, tiled=True)
    gate_act = jnp.dot(shard_piece, gate_rows, preferred_element_type=jnp.float32)
    up_act = jnp.dot(shard_piece, up_rows, preferred_element_type=jnp.float32)
    hidden = activate(gate_act, up_act)
    part_sum = jnp.dot(hidden, down_rows, preferred_element_type=jnp.float32)
    reduced = lax.psum_scatter(part_sum, "mp", scatter_dimension=1, tiled=True).astype(jnp.bfloat16)
    out_width = reduced.shape[1]
    returned = lax.all_to_all(
        reduced.reshape(senders, most_rows, out_width),
        "expert",
        split_axis=0,
        concat_axis=0,
        tiled=True,
    )
    summed = jnp.sum(
        returned.reshape(EXPERTS, group_size, most_rows, out_width).astype(jnp.float32), axis=1
    )
    result = jnp.dot(
        combine_w, summed.reshape(EXPERTS * most_rows, out_width), precision=lax.Precision.HIGHEST
    )
    return result.astype(jnp.bfloat16)


def solution(mesh):
    placed = (
        P("expert", "mp"),
        P("expert", None),
        P("expert", None),
        P("expert", None, "mp"),
        P("expert", None, "mp"),
        P("expert", "mp", None),
    )
    return jax.shard_map(
        local_any, mesh=mesh, in_specs=placed, out_specs=P("expert", "mp"), check_vma=False
    )
```
